32 devices in a mesh: rows: 8 (over z, y), cols: 4 (over x, core).
Axes of the slice: x: 2, y: 2, z: 4, core: 2. Of those that a mesh axis runs over, the one named last changes fastest.
Arguments:
- weight_up: bfloat16 [12288, 49152], P('rows', 'cols'), may hold values from -0.078125 to 0.078125
- low_up: bfloat16 [12288, 64], P('rows'), may hold values from -0.0546875 to 0.0546875
- high_up: bfloat16 [64, 49152], P(None, 'cols'), may hold values from -0.75 to 0.75
- norm_train: float32 [12288], P(('rows', 'cols')), may hold values from 0.25 to 1.75
- norm_step: float32 [12288], P(('rows', 'cols')), may hold values from -0.3 to 0.3
Outputs:
- serve_up: bfloat16 [12288, 49152], P(None, ('cols', 'rows'))
- scale_up: float32 [49152], P(('cols', 'rows'))
- serve_norm: bfloat16 [12288], replicated
The draws below stay inside these ranges and needn't reach their ends.
All inputs are finite; a program needn't handle non-finite values.
Results may differ from the reference program's by a relative error of at most 0.0004.
Values may be sent and summed in bfloat16 or wider, within the bound.
A program may use at most 256 MiB of HBM per device.

```python
import jax
import jax.numpy as jnp
from jax import lax

D_MODEL = 12288
D_INNER = 49152
RANK = 64


def raised(array, own_key, source, target, parts, factor):
    owner, partner = [(jnp.arange(array.shape[position]) // (array.shape[position] // parts)).reshape([-1 if axis == position else 1 for axis in range(array.ndim)]) for position in (source, target)]
    chosen = jax.random.permutation(own_key, parts)[partner]
    strong = (owner == chosen) | (owner == (partner + parts // 2) % parts)
    return jnp.where(strong, factor * array, array)


def shard_levels(own_key, shape, cuts, smallest, largest):
    level = 1.0
    for position, shards_of in cuts:
        draws = jax.random.uniform(jax.random.fold_in(jax.random.fold_in(own_key, 6), position), (shards_of,), jnp.float32, smallest / len(cuts), largest / len(cuts))
        level = level * jnp.repeat(jnp.exp(draws), shape[position] // shards_of).reshape((-1,) + (1,) * (len(shape) - 1 - position))
    return level


def gaussian(own_key, dims, width, limit, cuts=(), held_as=jnp.bfloat16):
    array = jax.random.normal(own_key, dims, jnp.float32) * width
    if len(cuts) > 0:
        array = shard_levels(own_key, dims, cuts, -0.22, 0.18) * array
    return jnp.clip(array, min=-limit, max=limit).astype(held_as)


def heavy_noise(key, dims, deviation, reach, shards, heavy, held_as=jnp.bfloat16):
    entries = deviation * jax.random.normal(key, dims, jnp.float32)
    if shards:
        entries = entries * shard_levels(key, dims, shards, -0.22, 0.18)
    return jnp.clip(raised(entries, jax.random.fold_in(key, 3), *heavy), -reach, reach).astype(held_as)


def setup_inputs(seed: int = 0) -> dict:
    key_of = jax.random.split(jax.random.key(seed), 6)
    return {
        "weight_up": heavy_noise(key_of[0], (D_MODEL, D_INNER), D_MODEL ** -0.5, 0.078125, ((0, 8), (1, 4)), (0, 1, 8, 2.0)),
        "low_up": gaussian(key_of[1], (D_MODEL, RANK), D_MODEL ** -0.5, 0.0546875, ((0, 8),)),
        "high_up": gaussian(key_of[2], (RANK, D_INNER), RANK ** -0.5, 0.75, ((1, 4),)),
        "norm_train": jnp.clip(1.0 + 0.15 * jax.random.normal(key_of[3], (D_MODEL,), jnp.float32), 0.25, 1.75),
        "norm_step": jnp.clip(jax.random.uniform(key_of[4], (D_MODEL,), jnp.float32, -0.3, 0.3) * shard_levels(key_of[4], (D_MODEL,), ((0, 32),), -0.4, 0.0), -0.3, 0.3),
    }


mix_rate = 0.5

def reference(weight_up, low_up, high_up, norm_train, norm_step):
    fresh_up = weight_up.astype(jnp.float32) + mix_rate * jnp.dot(low_up, high_up, preferred_element_type=jnp.float32)
    scale_up = jnp.sqrt(lax.optimization_barrier(jnp.sum(fresh_up * fresh_up, axis=0)))
    serve_up = (fresh_up / scale_up).astype(jnp.bfloat16)
    serve_norm = (norm_train + norm_step).astype(jnp.bfloat16)
    return (serve_up, scale_up, serve_norm)
```

```python
import functools

import jax
import jax.numpy as jnp
from jax import lax
from jax.experimental import pallas as pl
from jax.experimental.pallas import tpu as pltpu
from jax.sharding import PartitionSpec as P

mix_rate = 0.5
MESH = pl.DeviceIdType.MESH
LANES = 128


def partner(me, step):
    bit, other = 1, me
    while bit <= step:
        if step & bit:
            other = other + bit - 2 * bit * lax.rem(other // bit, 2)
        bit *= 2
    return other


def send_orders(ranks):
    far, near = list(range(ranks - 1, ranks // 2 - 1, -1)), list(range(ranks // 2 - 1, 0, -1))
    half = len(far) // 2
    turned = near[:-1][::-1] + near[-1:]
    return far + near, far[half:] + far[:half] + turned


def exchange(
    ranks, teams, w_ref, low_ref, high_ref, train_ref, step_ref,
    held, scale_out, norm_out,
    scale_ref, norm_ref, small_sem, fresh, norm_all, norms, low_all, high_own,
    send_sem, recv_sem, own_sem, high_sem,
    low_send, low_recv, low_own, norm_send, norm_recv, norm_own,
    low_send2, low_recv2, norm_send2, norm_recv2,
):
    me, team = lax.axis_index("rows"), lax.axis_index("cols")
    rows, columns = w_ref.shape
    share = columns // ranks
    pieces = share // LANES
    part = rows // teams
    half = ranks // 2
    parity = lax.rem(team, 2)
    gains = (train_ref, step_ref)

    def pick(first, second):
        first, second = partner(me, first), partner(me, second)
        return first + parity * (second - first)

    peers = [pick(first, second) for first, second in zip(*send_orders(ranks))]
    arrivals = peers[half:][::-1] + peers[:half]

    def window(owner, piece):
        return pl.ds(pl.multiple_of(owner * share + piece * LANES, LANES), LANES)

    def block(owner):
        return pl.ds(pl.multiple_of(owner * rows, 16), rows)

    def piece_copy(piece, to, source_rank):
        return pltpu.make_async_remote_copy(
            src_ref=w_ref.at[:, window(to, piece)],
            dst_ref=held.at[piece, block(me)],
            send_sem=send_sem.at[piece, to],
            recv_sem=recv_sem.at[piece, source_rank],
            device_id={"rows": to},
            device_id_type=MESH,
        )

    def piece_own(piece):
        return pltpu.make_async_copy(
            w_ref.at[:, window(me, piece)], held.at[piece, block(me)], own_sem.at[piece]
        )

    def issue(piece):
        for to in peers:
            piece_copy(piece, to, me).start()
        piece_own(piece).start()

    low_mine = low_ref.at[:, pl.ds(pl.multiple_of(team * part, LANES), part)]

    def low_copy(source, owner, to, sem):
        return pltpu.make_async_remote_copy(
            src_ref=source,
            dst_ref=low_all.at[team, owner],
            send_sem=low_send.at[sem],
            recv_sem=low_recv.at[owner],
            device_id={"rows": to},
            device_id_type=MESH,
        )

    def norm_copy(which, to, source_rank):
        return pltpu.make_async_remote_copy(
            src_ref=gains[which],
            dst_ref=norm_all.at[which, team, me],
            send_sem=norm_send.at[which, to],
            recv_sem=norm_recv.at[which, source_rank],
            device_id={"rows": to},
            device_id_type=MESH,
        )

    def team_copy(buffer, sends, receives, to, source_team):
        return pltpu.make_async_remote_copy(
            src_ref=buffer.at[team],
            dst_ref=buffer.at[team],
            send_sem=sends.at[to],
            recv_sem=receives.at[source_team],
            device_id={"cols": to},
            device_id_type=MESH,
        )

    high_copy = pltpu.make_async_copy(
        high_ref.at[:, pl.ds(pl.multiple_of(me * share, LANES), share)], high_own, high_sem
    )
    high_copy.start()
    low_keep = pltpu.make_async_copy(low_mine, low_all.at[team, me], low_own)
    low_keep.start()
    norm_keep = [
        pltpu.make_async_copy(gains[which], norm_all.at[which, team, me], norm_own.at[which])
        for which in range(2)
    ]
    for copy in norm_keep:
        copy.start()

    barrier = pltpu.get_barrier_semaphore()
    for step in range(1, ranks):
        pl.semaphore_signal(
            barrier, inc=1, device_id={"rows": partner(me, step)}, device_id_type=MESH
        )
    for step in range(1, teams):
        pl.semaphore_signal(
            barrier, inc=1, device_id={"cols": lax.rem(team + step, teams)}, device_id_type=MESH
        )
    pl.semaphore_wait(barrier, ranks - 1 + teams - 1)

    across = partner(me, half)
    direct = [half] + list(range(1, half))
    for step in direct:
        low_copy(low_mine, me, partner(me, step), step).start()
    for step in range(1, ranks):
        for which in range(2):
            norm_copy(which, partner(me, step), me).start()

    issue(0)

    low_copy(low_mine, across, across, half).wait_recv()
    for step in range(1, half):
        low_copy(low_all.at[team, across], across, partner(me, step), half + step).start()

    @pl.loop(1, pieces)
    def _(piece):
        issue(piece)

    low_keep.wait()
    for copy in norm_keep:
        copy.wait()
    for step in direct:
        low_copy(low_mine, me, partner(me, step), step).wait_send()
    for step in range(1, half):
        low_copy(low_mine, partner(me, step), across, step).wait_recv()
        low_copy(low_mine, partner(me, half + step), across, step).wait_recv()
        low_copy(low_all.at[team, across], across, partner(me, step), half + step).wait_send()
    for step in range(1, ranks):
        for which in range(2):
            norm_copy(which, partner(me, step), partner(me, step)).wait()
    high_copy.wait()

    gathers = [(low_all, low_send2, low_recv2)] + [
        (norm_all.at[which], norm_send2.at[which], norm_recv2.at[which]) for which in range(2)
    ]
    for step in range(1, teams):
        for gather in gathers:
            team_copy(*gather, lax.rem(team + step, teams), team).start()
    for step in range(1, teams):
        to, back = lax.rem(team + step, teams), lax.rem(team + teams - step, teams)
        for gather in gathers:
            team_copy(*gather, to, back).wait()

    height = train_ref.shape[0]
    for rank in range(ranks):
        for mate in range(teams):
            at = (rank * teams + mate) * height
            norms[at:at + height, :] = norm_all[0, mate, rank] + norm_all[1, mate, rank]
    norm_ref[...] = norms[...].astype(jnp.bfloat16)
    norm_put = pltpu.make_async_copy(norm_ref, norm_out, small_sem.at[1])
    norm_put.start()

    def gather_block(piece, owner, total):
        high = high_own[:, pl.ds(pl.multiple_of(piece * LANES, LANES), LANES)]

        def one(quarter, total):
            added = lax.dot_general(
                low_all[quarter, owner], high, (((0,), (0,)), ((), ())),
                preferred_element_type=jnp.float32,
            )
            span = pl.ds(pl.multiple_of(owner * rows + quarter * part, 16), part)
            now = held[piece, span, :].astype(jnp.float32) + mix_rate * added
            fresh[span, :] = now
            return total + jnp.sum((now * now).reshape(part // 8, 8, LANES), axis=0)

        return lax.fori_loop(0, teams, one, total)

    def gather(piece):
        piece_own(piece).wait()
        total = gather_block(piece, me, jnp.zeros((8, LANES), jnp.float32))
        for back in arrivals:
            piece_copy(piece, back, back).wait_recv()
            total = gather_block(piece, back, total)
        scale = jnp.sqrt(jnp.sum(total, axis=0, keepdims=True))
        scale_ref[pl.ds(piece, 1), :] = scale
        return scale

    @pl.loop(0, pieces)
    def _(piece):
        inverse = 1.0 / gather(piece)

        @pl.loop(0, ranks * teams)
        def _(index):
            span = pl.ds(pl.multiple_of(index * part, 16), part)
            held[piece, span, :] = (fresh[span, :] * inverse).astype(jnp.bfloat16)

    scale_put = pltpu.make_async_copy(scale_ref, scale_out, small_sem.at[0])
    scale_put.start()

    @pl.loop(0, pieces)
    def _(piece):
        for to in peers:
            piece_copy(piece, to, me).wait_send()
    norm_put.wait()
    scale_put.wait()


def write_out(held, serve_ref, out_sem):
    copies = [
        pltpu.make_async_copy(
            held.at[piece], serve_ref.at[:, pl.ds(piece * LANES, LANES)], out_sem.at[piece]
        )
        for piece in range(held.shape[0])
    ]
    for copy in copies:
        copy.start()
    for copy in copies:
        copy.wait()


def with_kernel(ranks, teams, weight_up, low_up, high_up, norm_train, norm_step):
    rows, columns = weight_up.shape
    rank = low_up.shape[1]
    share = columns // ranks
    pieces = share // LANES
    part = rows // teams
    height = norm_train.shape[0] // LANES
    dma = pltpu.SemaphoreType.DMA
    anywhere, vmem = pl.BlockSpec(memory_space=pl.ANY), pl.BlockSpec(memory_space=pltpu.VMEM)
    shapes = (
        ((ranks * rows, share), jnp.bfloat16),
        ((pieces, LANES), jnp.float32),
        ((ranks * teams * height, LANES), jnp.bfloat16),
    )
    held, scale_up, serve_norm = pl.pallas_call(
        functools.partial(exchange, ranks, teams),
        out_shape=(
            pltpu.VMEM((pieces, ranks * rows, LANES), jnp.bfloat16),
            *[jax.ShapeDtypeStruct(*shape) for shape in shapes[1:]],
        ),
        in_specs=[anywhere] * 5,
        out_specs=(vmem, anywhere, anywhere),
        scratch_shapes=[
            *[pltpu.VMEM(*shape) for shape in shapes[1:]],
            dma((2,)),
            pltpu.VMEM((ranks * rows, LANES), jnp.float32),
            pltpu.VMEM((2, teams, ranks, height, LANES), jnp.float32),
            pltpu.VMEM((ranks * teams * height, LANES), jnp.float32),
            pltpu.VMEM((teams, ranks, rank, part), jnp.bfloat16),
            pltpu.VMEM((rank, share), jnp.bfloat16),
            dma((pieces, ranks)), dma((pieces, ranks)), dma((pieces,)), dma,
            dma((2 * ranks,)), dma((ranks,)), dma, dma((2, ranks)), dma((2, ranks)), dma((2,)),
            dma((teams,)), dma((teams,)), dma((2, teams)), dma((2, teams)),
        ],
        compiler_params=pltpu.CompilerParams(
            collective_id=0, has_side_effects=True, vmem_limit_bytes=20 * 1024 * 1024
        ),
    )(
        weight_up, low_up.T, high_up,
        norm_train.reshape(height, LANES), norm_step.reshape(height, LANES),
    )
    serve_up = pl.pallas_call(
        write_out,
        out_shape=jax.ShapeDtypeStruct(*shapes[0]),
        in_specs=[anywhere],
        out_specs=anywhere,
        scratch_shapes=[dma((pieces,))],
        compiler_params=pltpu.CompilerParams(vmem_limit_bytes=1024 * 1024),
    )(held)
    return serve_up, scale_up.reshape(-1), serve_norm.reshape(-1)


def with_collectives(weight_up, low_up, high_up, norm_train, norm_step):
    fresh_up = weight_up.astype(jnp.float32) + mix_rate * jnp.dot(
        low_up, high_up, preferred_element_type=jnp.float32
    )
    total_up = lax.psum(jnp.sum(fresh_up * fresh_up, axis=0), "rows")
    scale_up = jnp.sqrt(total_up)
    narrow_up = (fresh_up / scale_up).astype(jnp.bfloat16)
    serve_up = lax.all_to_all(narrow_up, "rows", split_axis=1, concat_axis=0, tiled=True)
    place = lax.axis_index("rows")
    scale_up = lax.dynamic_slice_in_dim(scale_up, place * serve_up.shape[1], serve_up.shape[1])
    serve_norm = lax.all_gather(
        (norm_train + norm_step).astype(jnp.bfloat16), ("rows", "cols"), axis=0, tiled=True
    )
    return (serve_up, scale_up, serve_norm)


def solution(mesh):
    ranks, teams = mesh.shape["rows"], mesh.shape["cols"]

    def per_device(weight_up, low_up, high_up, norm_train, norm_step):
        rows, columns = weight_up.shape
        share = columns // ranks
        aligned = (
            share % LANES == 0 and rows % (LANES * teams) == 0
            and ranks & (ranks - 1) == 0 and norm_train.shape[0] % LANES == 0
        )
        fits = 2 * ranks * rows * share < 40 * 1024 * 1024
        if aligned and fits:
            return with_kernel(ranks, teams, weight_up, low_up, high_up, norm_train, norm_step)
        return with_collectives(weight_up, low_up, high_up, norm_train, norm_step)

    in_specs = (
        P("rows", "cols"),
        P("rows", None),
        P(None, "cols"),
        P(("rows", "cols")),
        P(("rows", "cols")),
    )
    out_specs = (P(None, ("cols", "rows")), P(("cols", "rows")), P())
    return jax.shard_map(
        per_device, mesh=mesh, in_specs=in_specs, out_specs=out_specs, check_vma=False
    )
```

```python
import functools

import jax
import jax.numpy as jnp
from jax import lax
from jax.experimental import pallas as pl
from jax.experimental.pallas import tpu as pltpu
from jax.sharding import PartitionSpec as P

mix_rate = 0.5
MESH = pl.DeviceIdType.MESH
LANES = 128


def partner(me, step):
    bit, other = 1, me
    while bit <= step:
        if step & bit:
            other = other + bit - 2 * bit * lax.rem(other // bit, 2)
        bit *= 2
    return other


def send_orders(ranks):
    far, near = list(range(ranks - 1, ranks // 2 - 1, -1)), list(range(ranks // 2 - 1, 0, -1))
    half = len(far) // 2
    turned = near[:-1][::-1] + near[-1:]
    return far + near, far[half:] + far[:half] + turned


def cut(pieces):
    return pieces - 2 + lax.rem(lax.axis_index("cols"), 2)


def exchange(ranks, teams, first, *refs):
    if first:
        (
            w_ref, low_ref, high_ref, train_ref, step_ref,
            held, scale_out, low_out, norm_out,
            scale_ref, small_sem, fresh, low_all, high_own, send_sem, recv_sem, own_sem, high_sem,
            norm_ref, norm_all, norms,
            low_send, low_recv, low_own, norm_send, norm_recv, norm_own,
            low_send2, low_recv2, norm_send2, norm_recv2,
        ) = refs
        gains = (train_ref, step_ref)
    else:
        (
            w_ref, low_ref, high_ref, scale_in,
            held, scale_out,
            scale_ref, small_sem, fresh, low_all, high_own, send_sem, recv_sem, own_sem, high_sem,
        ) = refs
    me, team = lax.axis_index("rows"), lax.axis_index("cols")
    rows, columns = w_ref.shape
    share = columns // ranks
    pieces = share // LANES
    part = rows // teams
    half = ranks // 2
    parity = lax.rem(team, 2)
    low, high = (0, cut(pieces)) if first else (cut(pieces), pieces)

    def pick(one, other):
        one, other = partner(me, one), partner(me, other)
        return one + parity * (other - one)

    peers = [pick(one, other) for one, other in zip(*send_orders(ranks))]
    arrivals = peers[half:][::-1] + peers[:half]

    def window(owner, piece):
        return pl.ds(pl.multiple_of(owner * share + piece * LANES, LANES), LANES)

    def block(owner):
        return pl.ds(pl.multiple_of(owner * rows, 16), rows)

    def piece_copy(piece, to, source_rank):
        return pltpu.make_async_remote_copy(
            src_ref=w_ref.at[:, window(to, piece)],
            dst_ref=held.at[piece - low, block(me)],
            send_sem=send_sem.at[piece - low, to],
            recv_sem=recv_sem.at[piece - low, source_rank],
            device_id={"rows": to},
            device_id_type=MESH,
        )

    def piece_own(piece):
        return pltpu.make_async_copy(
            w_ref.at[:, window(me, piece)], held.at[piece - low, block(me)], own_sem.at[piece - low]
        )

    def issue(piece):
        for to in peers:
            piece_copy(piece, to, me).start()
        piece_own(piece).start()

    high_copy = pltpu.make_async_copy(
        high_ref.at[:, pl.ds(pl.multiple_of(me * share, LANES), share)], high_own, high_sem
    )
    high_copy.start()

    def greet(mates):
        barrier = pltpu.get_barrier_semaphore()
        for step in range(1, ranks):
            pl.semaphore_signal(
                barrier, inc=1, device_id={"rows": partner(me, step)}, device_id_type=MESH
            )
        for step in range(1, mates):
            pl.semaphore_signal(
                barrier, inc=1, device_id={"cols": lax.rem(team + step, mates)},
                device_id_type=MESH,
            )
        pl.semaphore_wait(barrier, ranks - 1 + mates - 1)

    def start_first():
        low_mine = low_ref.at[:, pl.ds(pl.multiple_of(team * part, LANES), part)]

        def low_copy(source, owner, to, sem):
            return pltpu.make_async_remote_copy(
                src_ref=source,
                dst_ref=low_all.at[team, owner],
                send_sem=low_send.at[sem],
                recv_sem=low_recv.at[owner],
                device_id={"rows": to},
                device_id_type=MESH,
            )

        def norm_copy(which, to, source_rank):
            return pltpu.make_async_remote_copy(
                src_ref=gains[which],
                dst_ref=norm_all.at[which, team, me],
                send_sem=norm_send.at[which, to],
                recv_sem=norm_recv.at[which, source_rank],
                device_id={"rows": to},
                device_id_type=MESH,
            )

        def team_copy(buffer, sends, receives, to, source_team):
            return pltpu.make_async_remote_copy(
                src_ref=buffer.at[team],
                dst_ref=buffer.at[team],
                send_sem=sends.at[to],
                recv_sem=receives.at[source_team],
                device_id={"cols": to},
                device_id_type=MESH,
            )

        keeps = [pltpu.make_async_copy(low_mine, low_all.at[team, me], low_own)] + [
            pltpu.make_async_copy(gains[which], norm_all.at[which, team, me], norm_own.at[which])
            for which in range(2)
        ]
        for copy in keeps:
            copy.start()
        greet(teams)

        across = partner(me, half)
        direct = [half] + list(range(1, half))
        for step in direct:
            low_copy(low_mine, me, partner(me, step), step).start()
        for step in range(1, ranks):
            for which in range(2):
                norm_copy(which, partner(me, step), me).start()

        issue(low)

        low_copy(low_mine, across, across, half).wait_recv()
        for step in range(1, half):
            low_copy(low_all.at[team, across], across, partner(me, step), half + step).start()

        pl.loop(low + 1, high)(issue)

        for copy in keeps:
            copy.wait()
        for step in direct:
            low_copy(low_mine, me, partner(me, step), step).wait_send()
        for step in range(1, half):
            low_copy(low_mine, partner(me, step), across, step).wait_recv()
            low_copy(low_mine, partner(me, half + step), across, step).wait_recv()
            low_copy(low_all.at[team, across], across, partner(me, step), half + step).wait_send()
        for step in range(1, ranks):
            for which in range(2):
                norm_copy(which, partner(me, step), partner(me, step)).wait()
        high_copy.wait()

        gathers = [(low_all, low_send2, low_recv2)] + [
            (norm_all.at[which], norm_send2.at[which], norm_recv2.at[which]) for which in range(2)
        ]
        for step in range(1, teams):
            for gather in gathers:
                team_copy(*gather, lax.rem(team + step, teams), team).start()
        for step in range(1, teams):
            to, back = lax.rem(team + step, teams), lax.rem(team + teams - step, teams)
            for gather in gathers:
                team_copy(*gather, to, back).wait()

        height = train_ref.shape[0]
        for rank in range(ranks):
            for mate in range(teams):
                at = (rank * teams + mate) * height
                norms[at:at + height, :] = norm_all[0, mate, rank] + norm_all[1, mate, rank]
        norm_ref[...] = norms[...].astype(jnp.bfloat16)
        puts = [
            pltpu.make_async_copy(low_all, low_out, small_sem.at[1]),
            pltpu.make_async_copy(norm_ref, norm_out, small_sem.at[2]),
        ]
        for copy in puts:
            copy.start()
        return puts

    def start_second():
        takes = [
            high_copy,
            pltpu.make_async_copy(low_ref, low_all, small_sem.at[1]),
            pltpu.make_async_copy(scale_in, scale_ref, small_sem.at[2]),
        ]
        for copy in takes[1:]:
            copy.start()
        greet(1)
        pl.loop(low, high)(issue)
        for copy in takes:
            copy.wait()
        return []

    puts = start_first() if first else start_second()

    def gather_block(piece, owner, total):
        now_high = high_own[:, pl.ds(pl.multiple_of(piece * LANES, LANES), LANES)]

        def one(quarter, total):
            added = lax.dot_general(
                low_all[quarter, owner], now_high, (((0,), (0,)), ((), ())),
                preferred_element_type=jnp.float32,
            )
            span = pl.ds(pl.multiple_of(owner * rows + quarter * part, 16), part)
            now = held[piece - low, span, :].astype(jnp.float32) + mix_rate * added
            fresh[span, :] = now
            return total + jnp.sum((now * now).reshape(part // 8, 8, LANES), axis=0)

        return lax.fori_loop(0, teams, one, total)

    @pl.loop(low, high)
    def _(piece):
        piece_own(piece).wait()
        total = gather_block(piece, me, jnp.zeros((8, LANES), jnp.float32))
        for back in arrivals:
            piece_copy(piece, back, back).wait_recv()
            total = gather_block(piece, back, total)
        scale = jnp.sqrt(jnp.sum(total, axis=0, keepdims=True))
        scale_ref[pl.ds(piece, 1), :] = scale
        inverse = 1.0 / scale

        @pl.loop(0, ranks * teams)
        def _(index):
            span = pl.ds(pl.multiple_of(index * part, 16), part)
            held[piece - low, span, :] = (fresh[span, :] * inverse).astype(jnp.bfloat16)

    scale_put = pltpu.make_async_copy(scale_ref, scale_out, small_sem.at[0])
    scale_put.start()

    @pl.loop(low, high)
    def _(piece):
        for to in peers:
            piece_copy(piece, to, me).wait_send()

    scale_put.wait()
    for copy in puts:
        copy.wait()


def window_of(piece):
    return pl.ds(piece * LANES, LANES)


def write_first(held, scale_ref, norm_ref, serve_ref, scale_out, norm_out, out_sem, small_sem):
    pieces = held.shape[0] + 1
    puts = [
        pltpu.make_async_copy(
            held.at[piece], serve_ref.at[:, window_of(piece)], out_sem.at[piece]
        )
        for piece in range(pieces - 1)
    ]
    smalls = [
        pltpu.make_async_copy(scale_ref, scale_out, small_sem.at[0]),
        pltpu.make_async_copy(norm_ref, norm_out, small_sem.at[1]),
    ]
    late = cut(pieces) == pieces - 1
    for copy in smalls + puts[:-1]:
        copy.start()
    pl.when(late)(puts[-1].start)
    for copy in smalls + puts[:-1]:
        copy.wait()
    pl.when(late)(puts[-1].wait)


def write_second(pieces, _, held, scale_ref, serve_ref, scale_out, out_sem, small_sem):
    early = cut(pieces) == pieces - 2
    middle = pltpu.make_async_copy(
        held.at[0], serve_ref.at[:, window_of(pieces - 2)], out_sem.at[0]
    )
    last = pltpu.make_async_copy(
        held.at[pieces - 1 - cut(pieces)], serve_ref.at[:, window_of(pieces - 1)], out_sem.at[1]
    )
    small = pltpu.make_async_copy(scale_ref, scale_out, small_sem)
    small.start()
    last.start()
    pl.when(early)(middle.start)
    small.wait()
    last.wait()
    pl.when(early)(middle.wait)


def with_kernel(ranks, teams, weight_up, low_up, high_up, norm_train, norm_step):
    rows, columns = weight_up.shape
    rank = low_up.shape[1]
    share = columns // ranks
    pieces = share // LANES
    part = rows // teams
    height = norm_train.shape[0] // LANES
    dma = pltpu.SemaphoreType.DMA
    anywhere, vmem = pl.BlockSpec(memory_space=pl.ANY), pl.BlockSpec(memory_space=pltpu.VMEM)
    hbm = pl.BlockSpec(memory_space=pltpu.HBM)

    def keep(*arrays):
        return [pltpu.with_memory_space_constraint(array, pltpu.HBM) for array in arrays]

    serve = jax.ShapeDtypeStruct((ranks * rows, share), jnp.bfloat16)
    scale = pltpu.HBM((pieces, LANES), jnp.float32)
    norm = pltpu.HBM((ranks * teams * height, LANES), jnp.bfloat16)
    lows = pltpu.HBM((teams, ranks, rank, part), jnp.bfloat16)

    def call(first, slots, outs, extra, *operands):
        return pl.pallas_call(
            functools.partial(exchange, ranks, teams, first),
            out_shape=(pltpu.VMEM((slots, ranks * rows, LANES), jnp.bfloat16), *outs),
            in_specs=[hbm] * len(operands),
            out_specs=(vmem, *[hbm] * len(outs)),
            scratch_shapes=[
                pltpu.VMEM(scale.shape, scale.dtype),
                dma((3,)),
                pltpu.VMEM((ranks * rows, LANES), jnp.float32),
                pltpu.VMEM(lows.shape, lows.dtype),
                pltpu.VMEM((rank, share), jnp.bfloat16),
                dma((slots, ranks)), dma((slots, ranks)), dma((slots,)), dma,
                *extra,
            ],
            compiler_params=pltpu.CompilerParams(
                collective_id=0 if first else 1, has_side_effects=True,
                vmem_limit_bytes=20 * 1024 * 1024,
            ),
        )(*keep(*operands))

    held, scale_up, low_all, serve_norm = call(
        True, pieces - 1, (scale, lows, norm),
        [
            pltpu.VMEM(norm.shape, norm.dtype),
            pltpu.VMEM((2, teams, ranks, height, LANES), jnp.float32),
            pltpu.VMEM(norm.shape, jnp.float32),
            dma((ranks,)), dma((ranks,)), dma, dma((2, ranks)), dma((2, ranks)), dma((2,)),
            dma((teams,)), dma((teams,)), dma((2, teams)), dma((2, teams)),
        ],
        weight_up, low_up.T, high_up,
        norm_train.reshape(height, LANES), norm_step.reshape(height, LANES),
    )
    serve_up, scale_up, serve_norm = pl.pallas_call(
        write_first,
        out_shape=(serve, scale, norm),
        in_specs=[anywhere, hbm, hbm],
        out_specs=(anywhere, hbm, hbm),
        scratch_shapes=[dma((pieces - 1,)), dma((2,))],
        compiler_params=pltpu.CompilerParams(vmem_limit_bytes=1024 * 1024),
    )(held, *keep(scale_up, serve_norm))
    held, scale_up = call(False, 2, (scale,), [], weight_up, low_all, high_up, scale_up)
    serve_up, scale_up = pl.pallas_call(
        functools.partial(write_second, pieces),
        out_shape=(serve, scale),
        in_specs=[anywhere, anywhere, hbm],
        out_specs=(anywhere, hbm),
        scratch_shapes=[dma((2,)), dma],
        compiler_params=pltpu.CompilerParams(vmem_limit_bytes=1024 * 1024),
        input_output_aliases={0: 0},
    )(serve_up, held, *keep(scale_up))
    return serve_up, scale_up.reshape(-1), serve_norm.reshape(-1)


def with_collectives(weight_up, low_up, high_up, norm_train, norm_step):
    fresh_up = weight_up.astype(jnp.float32) + mix_rate * jnp.dot(
        low_up, high_up, preferred_element_type=jnp.float32
    )
    total_up = lax.psum(jnp.sum(fresh_up * fresh_up, axis=0), "rows")
    scale_up = jnp.sqrt(total_up)
    narrow_up = (fresh_up / scale_up).astype(jnp.bfloat16)
    serve_up = lax.all_to_all(narrow_up, "rows", split_axis=1, concat_axis=0, tiled=True)
    place = lax.axis_index("rows")
    scale_up = lax.dynamic_slice_in_dim(scale_up, place * serve_up.shape[1], serve_up.shape[1])
    serve_norm = lax.all_gather(
        (norm_train + norm_step).astype(jnp.bfloat16), ("rows", "cols"), axis=0, tiled=True
    )
    return (serve_up, scale_up, serve_norm)


def solution(mesh):
    ranks, teams = mesh.shape["rows"], mesh.shape["cols"]

    def per_device(weight_up, low_up, high_up, norm_train, norm_step):
        rows, columns = weight_up.shape
        share = columns // ranks
        aligned = (
            share % LANES == 0 and share >= 3 * LANES and rows % (LANES * teams) == 0
            and ranks & (ranks - 1) == 0 and norm_train.shape[0] % LANES == 0
        )
        fits = 2 * ranks * rows * share < 40 * 1024 * 1024
        if aligned and fits:
            return with_kernel(ranks, teams, weight_up, low_up, high_up, norm_train, norm_step)
        return with_collectives(weight_up, low_up, high_up, norm_train, norm_step)

    in_specs = (
        P("rows", "cols"),
        P("rows", None),
        P(None, "cols"),
        P(("rows", "cols")),
        P(("rows", "cols")),
    )
    out_specs = (P(None, ("cols", "rows")), P(("cols", "rows")), P())
    return jax.shard_map(
        per_device, mesh=mesh, in_specs=in_specs, out_specs=out_specs, check_vma=False
    )
```

```python
import functools

import jax
import jax.numpy as jnp
from jax import lax
from jax.experimental import pallas as pl
from jax.experimental.pallas import tpu as pltpu
from jax.sharding import PartitionSpec as P

mix_rate = 0.5
MESH = pl.DeviceIdType.MESH
LANES = 128


def partner(me, step):
    bit, other = 1, me
    while bit <= step:
        if step & bit:
            other = other + bit - 2 * bit * lax.rem(other // bit, 2)
        bit *= 2
    return other


def send_orders(ranks):
    far, near = list(range(ranks - 1, ranks // 2 - 1, -1)), list(range(ranks // 2 - 1, 0, -1))
    half = len(far) // 2
    turned = near[:-1][::-1] + near[-1:]
    return far + near, far[half:] + far[:half] + turned


def cut(pieces):
    return pieces - 1 - lax.rem(lax.axis_index("cols"), 2)


def exchange(ranks, teams, first, *refs):
    if first:
        (
            w_ref, low_ref, high_ref, train_ref, step_ref,
            held, scale_out, low_out, norm_out,
            scale_ref, small_sem, fresh, low_all, high_own, send_sem, recv_sem, own_sem, high_sem,
            norm_ref, norm_all, norms,
            low_send, low_recv, low_own, norm_send, norm_recv, norm_own,
            low_send2, low_recv2, norm_send2, norm_recv2,
        ) = refs
        gains = (train_ref, step_ref)
    else:
        (
            w_ref, low_ref, high_ref, scale_in,
            held, scale_out,
            scale_ref, small_sem, fresh, low_all, high_own, send_sem, recv_sem, own_sem, high_sem,
        ) = refs
    me, team = lax.axis_index("rows"), lax.axis_index("cols")
    rows, columns = w_ref.shape
    share = columns // ranks
    pieces = share // LANES
    part = rows // teams
    half = ranks // 2
    parity = lax.rem(team, 2)
    low, high = (0, cut(pieces)) if first else (cut(pieces), pieces)

    def pick(one, other):
        one, other = partner(me, one), partner(me, other)
        return one + parity * (other - one)

    peers = [pick(one, other) for one, other in zip(*send_orders(ranks))]
    arrivals = peers[half:][::-1] + peers[:half]

    def window(owner, piece):
        return pl.ds(pl.multiple_of(owner * share + piece * LANES, LANES), LANES)

    def block(owner):
        return pl.ds(pl.multiple_of(owner * rows, 16), rows)

    def piece_copy(piece, to, source_rank):
        return pltpu.make_async_remote_copy(
            src_ref=w_ref.at[:, window(to, piece)],
            dst_ref=held.at[piece - low, block(me)],
            send_sem=send_sem.at[piece - low, to],
            recv_sem=recv_sem.at[piece - low, source_rank],
            device_id={"rows": to},
            device_id_type=MESH,
        )

    def piece_own(piece):
        return pltpu.make_async_copy(
            w_ref.at[:, window(me, piece)], held.at[piece - low, block(me)], own_sem.at[piece - low]
        )

    def issue(piece):
        for to in peers:
            piece_copy(piece, to, me).start()
        piece_own(piece).start()

    high_copy = pltpu.make_async_copy(
        high_ref.at[:, pl.ds(pl.multiple_of(me * share, LANES), share)], high_own, high_sem
    )
    high_copy.start()

    def greet(mates):
        barrier = pltpu.get_barrier_semaphore()
        for step in range(1, ranks):
            pl.semaphore_signal(
                barrier, inc=1, device_id={"rows": partner(me, step)}, device_id_type=MESH
            )
        for step in range(1, mates):
            pl.semaphore_signal(
                barrier, inc=1, device_id={"cols": lax.rem(team + step, mates)},
                device_id_type=MESH,
            )
        pl.semaphore_wait(barrier, ranks - 1 + mates - 1)

    def start_first():
        low_mine = low_ref.at[:, pl.ds(pl.multiple_of(team * part, LANES), part)]

        def low_copy(source, owner, to, sem):
            return pltpu.make_async_remote_copy(
                src_ref=source,
                dst_ref=low_all.at[team, owner],
                send_sem=low_send.at[sem],
                recv_sem=low_recv.at[owner],
                device_id={"rows": to},
                device_id_type=MESH,
            )

        def norm_copy(which, to, source_rank):
            return pltpu.make_async_remote_copy(
                src_ref=gains[which],
                dst_ref=norm_all.at[which, team, me],
                send_sem=norm_send.at[which, to],
                recv_sem=norm_recv.at[which, source_rank],
                device_id={"rows": to},
                device_id_type=MESH,
            )

        def team_copy(buffer, sends, receives, to, source_team):
            return pltpu.make_async_remote_copy(
                src_ref=buffer.at[team],
                dst_ref=buffer.at[team],
                send_sem=sends.at[to],
                recv_sem=receives.at[source_team],
                device_id={"cols": to},
                device_id_type=MESH,
            )

        keeps = [pltpu.make_async_copy(low_mine, low_all.at[team, me], low_own)] + [
            pltpu.make_async_copy(gains[which], norm_all.at[which, team, me], norm_own.at[which])
            for which in range(2)
        ]
        for copy in keeps:
            copy.start()
        greet(teams)

        across = partner(me, half)
        direct = [half] + list(range(1, half))
        for step in direct:
            low_copy(low_mine, me, partner(me, step), step).start()
        issue(low)
        for step in range(1, ranks):
            for which in range(2):
                norm_copy(which, partner(me, step), me).start()

        low_copy(low_mine, across, across, half).wait_recv()
        for step in range(1, half):
            low_copy(low_all.at[team, across], across, partner(me, step), half + step).start()

        pl.loop(low + 1, high)(issue)

        for copy in keeps:
            copy.wait()
        for step in direct:
            low_copy(low_mine, me, partner(me, step), step).wait_send()
        for step in range(1, half):
            low_copy(low_mine, partner(me, step), across, step).wait_recv()
            low_copy(low_mine, partner(me, half + step), across, step).wait_recv()
            low_copy(low_all.at[team, across], across, partner(me, step), half + step).wait_send()
        for step in range(1, ranks):
            for which in range(2):
                norm_copy(which, partner(me, step), partner(me, step)).wait()
        high_copy.wait()

        gathers = [(low_all, low_send2, low_recv2)] + [
            (norm_all.at[which], norm_send2.at[which], norm_recv2.at[which]) for which in range(2)
        ]
        for step in range(1, teams):
            for gather in gathers:
                team_copy(*gather, lax.rem(team + step, teams), team).start()
        for step in range(1, teams):
            to, back = lax.rem(team + step, teams), lax.rem(team + teams - step, teams)
            for gather in gathers:
                team_copy(*gather, to, back).wait()

        height = train_ref.shape[0]
        for rank in range(ranks):
            for mate in range(teams):
                at = (rank * teams + mate) * height
                norms[at:at + height, :] = norm_all[0, mate, rank] + norm_all[1, mate, rank]
        norm_ref[...] = norms[...].astype(jnp.bfloat16)
        puts = [
            pltpu.make_async_copy(low_all, low_out, small_sem.at[1]),
            pltpu.make_async_copy(norm_ref, norm_out, small_sem.at[2]),
        ]
        for copy in puts:
            copy.start()
        return puts

    def start_second():
        takes = [
            high_copy,
            pltpu.make_async_copy(low_ref, low_all, small_sem.at[1]),
            pltpu.make_async_copy(scale_in, scale_ref, small_sem.at[2]),
        ]
        for copy in takes[1:]:
            copy.start()
        greet(1)
        pl.loop(low, high)(issue)
        for copy in takes:
            copy.wait()
        return []

    puts = start_first() if first else start_second()

    def span(owner, quarter):
        return pl.ds(pl.multiple_of(owner * rows + quarter * part, 16), part)

    def prepare(piece):
        now_high = high_own[:, pl.ds(pl.multiple_of(piece * LANES, LANES), LANES)]

        @pl.loop(0, ranks)
        def _(owner):
            @pl.loop(0, teams)
            def _(quarter):
                fresh[span(owner, quarter), :] = mix_rate * lax.dot_general(
                    low_all[quarter, owner], now_high, (((0,), (0,)), ((), ())),
                    preferred_element_type=jnp.float32,
                )

    def gather_block(piece, owner, total):
        def one(quarter, total):
            at = span(owner, quarter)
            now = held[piece - low, at, :].astype(jnp.float32) + fresh[at, :]
            fresh[at, :] = now
            return total + jnp.sum((now * now).reshape(part // 8, 8, LANES), axis=0)

        return lax.fori_loop(0, teams, one, total)

    scale_put = pltpu.make_async_copy(scale_ref, scale_out, small_sem.at[0])

    @pl.loop(low, high)
    def _(piece):
        prepare(piece)
        piece_own(piece).wait()
        total = gather_block(piece, me, jnp.zeros((8, LANES), jnp.float32))
        for back in arrivals:
            piece_copy(piece, back, back).wait_recv()
            total = gather_block(piece, back, total)
        scale = jnp.sqrt(jnp.sum(total, axis=0, keepdims=True))
        scale_ref[pl.ds(piece, 1), :] = scale
        inverse = 1.0 / scale

        @pl.loop(0, ranks)
        def _(owner):
            @pl.loop(0, teams)
            def _(quarter):
                at = span(owner, quarter)
                held[piece - low, at, :] = (fresh[at, :] * inverse).astype(jnp.bfloat16)

            @pl.when(jnp.logical_and(piece == high - 1, owner == 0))
            def _():
                scale_put.start()

    @pl.loop(low, high)
    def _(piece):
        for to in peers:
            piece_copy(piece, to, me).wait_send()

    scale_put.wait()
    for copy in puts:
        copy.wait()


def window_of(piece):
    return pl.ds(piece * LANES, LANES)


def write_first(held, scale_ref, norm_ref, serve_ref, scale_out, norm_out, out_sem, small_sem):
    pieces = held.shape[0] + 1
    puts = [
        pltpu.make_async_copy(
            held.at[piece], serve_ref.at[:, window_of(piece)], out_sem.at[piece]
        )
        for piece in range(pieces - 1)
    ]
    smalls = [
        pltpu.make_async_copy(scale_ref, scale_out, small_sem.at[0]),
        pltpu.make_async_copy(norm_ref, norm_out, small_sem.at[1]),
    ]
    late = cut(pieces) == pieces - 1
    for copy in smalls + puts[:-1]:
        copy.start()
    pl.when(late)(puts[-1].start)
    for copy in smalls + puts[:-1]:
        copy.wait()
    pl.when(late)(puts[-1].wait)


def write_second(pieces, _, held, scale_ref, serve_ref, scale_out, out_sem, small_sem):
    early = cut(pieces) == pieces - 2
    middle = pltpu.make_async_copy(
        held.at[0], serve_ref.at[:, window_of(pieces - 2)], out_sem.at[0]
    )
    last = pltpu.make_async_copy(
        held.at[pieces - 1 - cut(pieces)], serve_ref.at[:, window_of(pieces - 1)], out_sem.at[1]
    )
    small = pltpu.make_async_copy(scale_ref, scale_out, small_sem)
    small.start()
    last.start()
    pl.when(early)(middle.start)
    small.wait()
    last.wait()
    pl.when(early)(middle.wait)


def with_kernel(ranks, teams, weight_up, low_up, high_up, norm_train, norm_step):
    rows, columns = weight_up.shape
    rank = low_up.shape[1]
    share = columns // ranks
    pieces = share // LANES
    part = rows // teams
    height = norm_train.shape[0] // LANES
    dma = pltpu.SemaphoreType.DMA
    anywhere, vmem = pl.BlockSpec(memory_space=pl.ANY), pl.BlockSpec(memory_space=pltpu.VMEM)
    hbm = pl.BlockSpec(memory_space=pltpu.HBM)

    def keep(*arrays):
        return [pltpu.with_memory_space_constraint(array, pltpu.HBM) for array in arrays]

    serve = jax.ShapeDtypeStruct((ranks * rows, share), jnp.bfloat16)
    scale = pltpu.HBM((pieces, LANES), jnp.float32)
    norm = pltpu.HBM((ranks * teams * height, LANES), jnp.bfloat16)
    lows = pltpu.HBM((teams, ranks, rank, part), jnp.bfloat16)

    def call(first, slots, outs, extra, *operands):
        return pl.pallas_call(
            functools.partial(exchange, ranks, teams, first),
            out_shape=(pltpu.VMEM((slots, ranks * rows, LANES), jnp.bfloat16), *outs),
            in_specs=[hbm] * len(operands),
            out_specs=(vmem, *[hbm] * len(outs)),
            scratch_shapes=[
                pltpu.VMEM(scale.shape, scale.dtype),
                dma((3,)),
                pltpu.VMEM((ranks * rows, LANES), jnp.float32),
                pltpu.VMEM(lows.shape, lows.dtype),
                pltpu.VMEM((rank, share), jnp.bfloat16),
                dma((slots, ranks)), dma((slots, ranks)), dma((slots,)), dma,
                *extra,
            ],
            compiler_params=pltpu.CompilerParams(
                collective_id=0 if first else 1, has_side_effects=True,
                vmem_limit_bytes=20 * 1024 * 1024,
            ),
        )(*keep(*operands))

    held, scale_up, low_all, serve_norm = call(
        True, pieces - 1, (scale, lows, norm),
        [
            pltpu.VMEM(norm.shape, norm.dtype),
            pltpu.VMEM((2, teams, ranks, height, LANES), jnp.float32),
            pltpu.VMEM(norm.shape, jnp.float32),
            dma((ranks,)), dma((ranks,)), dma, dma((2, ranks)), dma((2, ranks)), dma((2,)),
            dma((teams,)), dma((teams,)), dma((2, teams)), dma((2, teams)),
        ],
        weight_up, low_up.T, high_up,
        norm_train.reshape(height, LANES), norm_step.reshape(height, LANES),
    )
    serve_up, scale_up, serve_norm = pl.pallas_call(
        write_first,
        out_shape=(serve, scale, norm),
        in_specs=[anywhere, hbm, hbm],
        out_specs=(anywhere, hbm, hbm),
        scratch_shapes=[dma((pieces - 1,)), dma((2,))],
        compiler_params=pltpu.CompilerParams(vmem_limit_bytes=1024 * 1024),
    )(held, *keep(scale_up, serve_norm))
    held, scale_up = call(False, 2, (scale,), [], weight_up, low_all, high_up, scale_up)
    serve_up, scale_up = pl.pallas_call(
        functools.partial(write_second, pieces),
        out_shape=(serve, scale),
        in_specs=[anywhere, anywhere, hbm],
        out_specs=(anywhere, hbm),
        scratch_shapes=[dma((2,)), dma],
        compiler_params=pltpu.CompilerParams(vmem_limit_bytes=1024 * 1024),
        input_output_aliases={0: 0},
    )(serve_up, held, *keep(scale_up))
    return serve_up, scale_up.reshape(-1), serve_norm.reshape(-1)


def with_collectives(weight_up, low_up, high_up, norm_train, norm_step):
    fresh_up = weight_up.astype(jnp.float32) + mix_rate * jnp.dot(
        low_up, high_up, preferred_element_type=jnp.float32
    )
    total_up = lax.psum(jnp.sum(fresh_up * fresh_up, axis=0), "rows")
    scale_up = jnp.sqrt(total_up)
    narrow_up = (fresh_up / scale_up).astype(jnp.bfloat16)
    serve_up = lax.all_to_all(narrow_up, "rows", split_axis=1, concat_axis=0, tiled=True)
    place = lax.axis_index("rows")
    scale_up = lax.dynamic_slice_in_dim(scale_up, place * serve_up.shape[1], serve_up.shape[1])
    serve_norm = lax.all_gather(
        (norm_train + norm_step).astype(jnp.bfloat16), ("rows", "cols"), axis=0, tiled=True
    )
    return (serve_up, scale_up, serve_norm)


def solution(mesh):
    ranks, teams = mesh.shape["rows"], mesh.shape["cols"]

    def per_device(weight_up, low_up, high_up, norm_train, norm_step):
        rows, columns = weight_up.shape
        share = columns // ranks
        aligned = (
            share % LANES == 0 and share >= 3 * LANES and rows % (LANES * teams) == 0
            and ranks & (ranks - 1) == 0 and norm_train.shape[0] % LANES == 0
        )
        fits = 2 * ranks * rows * share < 40 * 1024 * 1024
        if aligned and fits:
            return with_kernel(ranks, teams, weight_up, low_up, high_up, norm_train, norm_step)
        return with_collectives(weight_up, low_up, high_up, norm_train, norm_step)

    in_specs = (
        P("rows", "cols"),
        P("rows", None),
        P(None, "cols"),
        P(("rows", "cols")),
        P(("rows", "cols")),
    )
    out_specs = (P(None, ("cols", "rows")), P(("cols", "rows")), P())
    return jax.shard_map(
        per_device, mesh=mesh, in_specs=in_specs, out_specs=out_specs, check_vma=False
    )
```

```python
import functools

import jax
import jax.numpy as jnp
from jax import lax
from jax.experimental import pallas as pl
from jax.experimental.pallas import tpu as pltpu
from jax.sharding import PartitionSpec as P

mix_rate = 0.5
MESH = pl.DeviceIdType.MESH
LANES = 128


def partner(me, step):
    bit, other = 1, me
    while bit <= step:
        if step & bit:
            other = other + bit - 2 * bit * lax.rem(me // bit, 2)
        bit *= 2
    return other


def send_orders(ranks, first):
    far, near = list(range(ranks - 1, ranks // 2 - 1, -1)), list(range(ranks // 2 - 1, 0, -1))
    half = len(far) // 2
    turned = near[:-1][::-1] + near[-1:]
    other = far[half:] + far[:half] + turned
    return (far + near if first else near + far), other


def cut(pieces):
    return pieces - 1 - lax.rem(lax.axis_index("cols"), 2)


def exchange(ranks, teams, first, *refs):
    if first:
        (
            w_ref, low_ref, high_ref, train_ref, step_ref,
            held, scale_out, low_out, norm_out,
            scale_ref, small_sem, fresh, low_all, high_own, send_sem, recv_sem, own_sem, high_sem,
            norm_ref, norm_all, norms,
            low_send, low_recv, low_own, norm_send, norm_recv, norm_own,
            low_send2, low_recv2, norm_send2, norm_recv2,
        ) = refs
        gains = (train_ref, step_ref)
    else:
        (
            w_ref, low_ref, high_ref, scale_in,
            held, scale_out,
            scale_ref, small_sem, fresh, low_all, high_own, send_sem, recv_sem, own_sem, high_sem,
        ) = refs
    me, team = lax.axis_index("rows"), lax.axis_index("cols")
    rows, columns = w_ref.shape
    share = columns // ranks
    pieces = share // LANES
    part = rows // teams
    half = ranks // 2
    parity = lax.rem(team, 2)
    low, high = (0, cut(pieces)) if first else (cut(pieces), pieces)

    def pick(one, other):
        one, other = partner(me, one), partner(me, other)
        return one + parity * (other - one)

    orders = send_orders(ranks, first)
    peers = [pick(one, other) for one, other in zip(*orders)]
    arrivals = [
        pick(one, other)
        for one, other in zip(
            *[sorted(order, key=lambda step: step >= half) for order in orders]
        )
    ]

    def window(owner, piece):
        return pl.ds(pl.multiple_of(owner * share + piece * LANES, LANES), LANES)

    def block(owner):
        return pl.ds(pl.multiple_of(owner * rows, 16), rows)

    def piece_copy(piece, to, source_rank):
        return pltpu.make_async_remote_copy(
            src_ref=w_ref.at[:, window(to, piece)],
            dst_ref=held.at[piece - low, block(me)],
            send_sem=send_sem.at[piece - low, to],
            recv_sem=recv_sem.at[piece - low, source_rank],
            device_id={"rows": to},
            device_id_type=MESH,
        )

    def piece_own(piece):
        return pltpu.make_async_copy(
            w_ref.at[:, window(me, piece)], held.at[piece - low, block(me)], own_sem.at[piece - low]
        )

    def issue(piece):
        for to in peers:
            piece_copy(piece, to, me).start()
        piece_own(piece).start()

    high_copy = pltpu.make_async_copy(
        high_ref.at[:, pl.ds(pl.multiple_of(me * share, LANES), share)], high_own, high_sem
    )
    high_copy.start()

    def greet(mates):
        barrier = pltpu.get_barrier_semaphore()
        for step in range(1, ranks):
            pl.semaphore_signal(
                barrier, inc=1, device_id={"rows": partner(me, step)}, device_id_type=MESH
            )
        for step in range(1, mates):
            pl.semaphore_signal(
                barrier, inc=1, device_id={"cols": lax.rem(team + step, mates)},
                device_id_type=MESH,
            )
        pl.semaphore_wait(barrier, ranks - 1 + mates - 1)

    def start_first():
        low_mine = low_ref.at[:, pl.ds(pl.multiple_of(team * part, LANES), part)]

        def low_copy(source, owner, to, sem):
            return pltpu.make_async_remote_copy(
                src_ref=source,
                dst_ref=low_all.at[team, owner],
                send_sem=low_send.at[sem],
                recv_sem=low_recv.at[owner],
                device_id={"rows": to},
                device_id_type=MESH,
            )

        def norm_copy(which, source, owner, to, sem):
            return pltpu.make_async_remote_copy(
                src_ref=source,
                dst_ref=norm_all.at[which, team, owner],
                send_sem=norm_send.at[which, sem],
                recv_sem=norm_recv.at[which, owner],
                device_id={"rows": to},
                device_id_type=MESH,
            )

        def own(to, sem, owner):
            return [low_copy(low_mine, owner, to, sem)] + [
                norm_copy(which, gains[which], owner, to, sem) for which in range(2)
            ]

        def passed_on(step):
            to, sem = partner(me, step), half + step
            return [low_copy(low_all.at[team, across], across, to, sem)] + [
                norm_copy(which, norm_all.at[which, team, across], across, to, sem)
                for which in range(2)
            ]

        def team_copy(buffer, sends, receives, to, source_team):
            return pltpu.make_async_remote_copy(
                src_ref=buffer.at[team],
                dst_ref=buffer.at[team],
                send_sem=sends.at[to],
                recv_sem=receives.at[source_team],
                device_id={"cols": to},
                device_id_type=MESH,
            )

        keeps = [pltpu.make_async_copy(low_mine, low_all.at[team, me], low_own)] + [
            pltpu.make_async_copy(gains[which], norm_all.at[which, team, me], norm_own.at[which])
            for which in range(2)
        ]
        for copy in keeps:
            copy.start()
        greet(teams)

        across = partner(me, half)
        direct = [half] + list(range(1, half))
        for step in direct:
            for copy in own(partner(me, step), step, me):
                copy.start()

        issue(low)

        for copy in own(across, half, across):
            copy.wait_recv()
        for step in range(1, half):
            for copy in passed_on(step):
                copy.start()

        pl.loop(low + 1, high)(issue)

        for copy in keeps:
            copy.wait()
        for step in direct:
            for copy in own(partner(me, step), step, me):
                copy.wait_send()
        for step in range(1, half):
            for owner in (partner(me, step), partner(me, half + step)):
                for copy in own(across, step, owner):
                    copy.wait_recv()
            for copy in passed_on(step):
                copy.wait_send()
        high_copy.wait()

        gathers = [(low_all, low_send2, low_recv2)] + [
            (norm_all.at[which], norm_send2.at[which], norm_recv2.at[which]) for which in range(2)
        ]
        for step in range(1, teams):
            for gather in gathers:
                team_copy(*gather, lax.rem(team + step, teams), team).start()
        for step in range(1, teams):
            to, back = lax.rem(team + step, teams), lax.rem(team + teams - step, teams)
            for gather in gathers:
                team_copy(*gather, to, back).wait()

        height = train_ref.shape[0]
        for rank in range(ranks):
            for mate in range(teams):
                at = (rank * teams + mate) * height
                norms[at:at + height, :] = norm_all[0, mate, rank] + norm_all[1, mate, rank]
        norm_ref[...] = norms[...].astype(jnp.bfloat16)
        puts = [
            pltpu.make_async_copy(low_all, low_out, small_sem.at[1]),
            pltpu.make_async_copy(norm_ref, norm_out, small_sem.at[2]),
        ]
        for copy in puts:
            copy.start()
        return puts

    def start_second():
        takes = [
            high_copy,
            pltpu.make_async_copy(low_ref, low_all, small_sem.at[1]),
            pltpu.make_async_copy(scale_in, scale_ref, small_sem.at[2]),
        ]
        for copy in takes[1:]:
            copy.start()
        greet(1)
        pl.loop(low, high)(issue)
        for copy in takes:
            copy.wait()
        return []

    puts = start_first() if first else start_second()

    def span(owner, quarter):
        return pl.ds(pl.multiple_of(owner * rows + quarter * part, 16), part)

    def prepare(piece):
        now_high = high_own[:, pl.ds(pl.multiple_of(piece * LANES, LANES), LANES)]

        @pl.loop(0, ranks)
        def _(owner):
            @pl.loop(0, teams)
            def _(quarter):
                fresh[span(owner, quarter), :] = mix_rate * lax.dot_general(
                    low_all[quarter, owner], now_high, (((0,), (0,)), ((), ())),
                    preferred_element_type=jnp.float32,
                )

    def gather_block(piece, owner, total):
        def one(quarter, total):
            at = span(owner, quarter)
            now = held[piece - low, at, :].astype(jnp.float32) + fresh[at, :]
            fresh[at, :] = now
            return total + jnp.sum((now * now).reshape(part // 8, 8, LANES), axis=0)

        return lax.fori_loop(0, teams, one, total)

    scale_put = pltpu.make_async_copy(scale_ref, scale_out, small_sem.at[0])

    @pl.loop(low, high)
    def _(piece):
        prepare(piece)
        piece_own(piece).wait()
        total = gather_block(piece, me, jnp.zeros((8, LANES), jnp.float32))
        for back in arrivals:
            piece_copy(piece, back, back).wait_recv()
            total = gather_block(piece, back, total)
        scale = jnp.sqrt(jnp.sum(total, axis=0, keepdims=True))
        scale_ref[pl.ds(piece, 1), :] = scale
        inverse = 1.0 / scale

        @pl.loop(0, ranks)
        def _(owner):
            @pl.loop(0, teams)
            def _(quarter):
                at = span(owner, quarter)
                held[piece - low, at, :] = (fresh[at, :] * inverse).astype(jnp.bfloat16)

            @pl.when(jnp.logical_and(piece == high - 1, owner == 0))
            def _():
                scale_put.start()

    @pl.loop(low, high)
    def _(piece):
        for to in peers:
            piece_copy(piece, to, me).wait_send()

    scale_put.wait()
    for copy in puts:
        copy.wait()


def window_of(piece):
    return pl.ds(piece * LANES, LANES)


def write_first(held, scale_ref, norm_ref, serve_ref, scale_out, norm_out, out_sem, small_sem):
    pieces = held.shape[0] + 1
    puts = [
        pltpu.make_async_copy(
            held.at[piece], serve_ref.at[:, window_of(piece)], out_sem.at[piece]
        )
        for piece in range(pieces - 1)
    ]
    smalls = [
        pltpu.make_async_copy(scale_ref, scale_out, small_sem.at[0]),
        pltpu.make_async_copy(norm_ref, norm_out, small_sem.at[1]),
    ]
    late = cut(pieces) == pieces - 1
    for copy in smalls + puts[:-1]:
        copy.start()
    pl.when(late)(puts[-1].start)
    for copy in smalls + puts[:-1]:
        copy.wait()
    pl.when(late)(puts[-1].wait)


def write_second(pieces, _, held, scale_ref, serve_ref, scale_out, out_sem, small_sem):
    early = cut(pieces) == pieces - 2
    middle = pltpu.make_async_copy(
        held.at[0], serve_ref.at[:, window_of(pieces - 2)], out_sem.at[0]
    )
    last = pltpu.make_async_copy(
        held.at[pieces - 1 - cut(pieces)], serve_ref.at[:, window_of(pieces - 1)], out_sem.at[1]
    )
    small = pltpu.make_async_copy(scale_ref, scale_out, small_sem)
    small.start()
    last.start()
    pl.when(early)(middle.start)
    small.wait()
    last.wait()
    pl.when(early)(middle.wait)


def with_kernel(ranks, teams, weight_up, low_up, high_up, norm_train, norm_step):
    rows, columns = weight_up.shape
    rank = low_up.shape[1]
    share = columns // ranks
    pieces = share // LANES
    part = rows // teams
    height = norm_train.shape[0] // LANES
    dma = pltpu.SemaphoreType.DMA
    anywhere, vmem = pl.BlockSpec(memory_space=pl.ANY), pl.BlockSpec(memory_space=pltpu.VMEM)
    hbm = pl.BlockSpec(memory_space=pltpu.HBM)

    def keep(*arrays):
        return [pltpu.with_memory_space_constraint(array, pltpu.HBM) for array in arrays]

    serve = jax.ShapeDtypeStruct((ranks * rows, share), jnp.bfloat16)
    scale = pltpu.HBM((pieces, LANES), jnp.float32)
    norm = pltpu.HBM((ranks * teams * height, LANES), jnp.bfloat16)
    lows = pltpu.HBM((teams, ranks, rank, part), jnp.bfloat16)

    def call(first, slots, outs, extra, *operands):
        return pl.pallas_call(
            functools.partial(exchange, ranks, teams, first),
            out_shape=(pltpu.VMEM((slots, ranks * rows, LANES), jnp.bfloat16), *outs),
            in_specs=[hbm] * len(operands),
            out_specs=(vmem, *[hbm] * len(outs)),
            scratch_shapes=[
                pltpu.VMEM(scale.shape, scale.dtype),
                dma((3,)),
                pltpu.VMEM((ranks * rows, LANES), jnp.float32),
                pltpu.VMEM(lows.shape, lows.dtype),
                pltpu.VMEM((rank, share), jnp.bfloat16),
                dma((slots, ranks)), dma((slots, ranks)), dma((slots,)), dma,
                *extra,
            ],
            compiler_params=pltpu.CompilerParams(
                collective_id=0 if first else 1, has_side_effects=True,
                vmem_limit_bytes=20 * 1024 * 1024,
            ),
        )(*keep(*operands))

    held, scale_up, low_all, serve_norm = call(
        True, pieces - 1, (scale, lows, norm),
        [
            pltpu.VMEM(norm.shape, norm.dtype),
            pltpu.VMEM((2, teams, ranks, height, LANES), jnp.float32),
            pltpu.VMEM(norm.shape, jnp.float32),
            dma((ranks,)), dma((ranks,)), dma, dma((2, ranks)), dma((2, ranks)), dma((2,)),
            dma((teams,)), dma((teams,)), dma((2, teams)), dma((2, teams)),
        ],
        weight_up, low_up.T, high_up,
        norm_train.reshape(height, LANES), norm_step.reshape(height, LANES),
    )
    serve_up, scale_up, serve_norm = pl.pallas_call(
        write_first,
        out_shape=(serve, scale, norm),
        in_specs=[anywhere, hbm, hbm],
        out_specs=(anywhere, hbm, hbm),
        scratch_shapes=[dma((pieces - 1,)), dma((2,))],
        compiler_params=pltpu.CompilerParams(vmem_limit_bytes=1024 * 1024),
    )(held, *keep(scale_up, serve_norm))
    held, scale_up = call(False, 2, (scale,), [], weight_up, low_all, high_up, scale_up)
    serve_up, scale_up = pl.pallas_call(
        functools.partial(write_second, pieces),
        out_shape=(serve, scale),
        in_specs=[anywhere, anywhere, hbm],
        out_specs=(anywhere, hbm),
        scratch_shapes=[dma((2,)), dma],
        compiler_params=pltpu.CompilerParams(vmem_limit_bytes=1024 * 1024),
        input_output_aliases={0: 0},
    )(serve_up, held, *keep(scale_up))
    return serve_up, scale_up.reshape(-1), serve_norm.reshape(-1)


def with_collectives(weight_up, low_up, high_up, norm_train, norm_step):
    fresh_up = weight_up.astype(jnp.float32) + mix_rate * jnp.dot(
        low_up, high_up, preferred_element_type=jnp.float32
    )
    total_up = lax.psum(jnp.sum(fresh_up * fresh_up, axis=0), "rows")
    scale_up = jnp.sqrt(total_up)
    narrow_up = (fresh_up / scale_up).astype(jnp.bfloat16)
    serve_up = lax.all_to_all(narrow_up, "rows", split_axis=1, concat_axis=0, tiled=True)
    place = lax.axis_index("rows")
    scale_up = lax.dynamic_slice_in_dim(scale_up, place * serve_up.shape[1], serve_up.shape[1])
    serve_norm = lax.all_gather(
        (norm_train + norm_step).astype(jnp.bfloat16), ("rows", "cols"), axis=0, tiled=True
    )
    return (serve_up, scale_up, serve_norm)


def solution(mesh):
    ranks, teams = mesh.shape["rows"], mesh.shape["cols"]

    def per_device(weight_up, low_up, high_up, norm_train, norm_step):
        rows, columns = weight_up.shape
        share = columns // ranks
        aligned = (
            share % LANES == 0 and share >= 3 * LANES and rows % (LANES * teams) == 0
            and ranks & (ranks - 1) == 0 and norm_train.shape[0] % LANES == 0
        )
        fits = 2 * ranks * rows * share < 40 * 1024 * 1024
        if aligned and fits:
            return with_kernel(ranks, teams, weight_up, low_up, high_up, norm_train, norm_step)
        return with_collectives(weight_up, low_up, high_up, norm_train, norm_step)

    in_specs = (
        P("rows", "cols"),
        P("rows", None),
        P(None, "cols"),
        P(("rows", "cols")),
        P(("rows", "cols")),
    )
    out_specs = (P(None, ("cols", "rows")), P(("cols", "rows")), P())
    return jax.shard_map(
        per_device, mesh=mesh, in_specs=in_specs, out_specs=out_specs, check_vma=False
    )
```
